32 devices in a mesh: batch: 4 (over z), row: 4 (over x, core), col: 2 (over y).
Axes of the slice: x: 2, y: 2, z: 4, core: 2. Of those that a mesh axis runs over, the one named last changes fastest.
Arguments:
- embeddings: bfloat16 [512, 128, 512], P('batch', 'col', 'row'), may hold values from -170 to 170
- projection: bfloat16 [512, 32], replicated, may hold values from -0.25 to 0.25
- w_in: bfloat16 [16384, 2048], P('row', 'col'), may hold values from -0.046875 to 0.046875
- bias: float32 [2048], P('col'), may hold values from -3 to 3
- w_out: bfloat16 [2048, 128, 512], P(None, 'col', 'row'), may hold values from -0.125 to 0.125
- cotangent: bfloat16 [512, 128, 512], P('batch', 'col', 'row'), may hold values from -0.1796875 to 0.1796875
Outputs:
- mixed: bfloat16 [512, 128, 512], P('batch', 'col', 'row')
- grad_out: float32 [2048, 128, 512], P('batch', 'col', 'row')
- grad_in: float32 [16384, 2048], P('row', 'col')
- grad_bias: float32 [2048], P('col')
- grad_proj: float32 [512, 32], P('row')
The draws below stay inside these ranges and needn't reach their ends.
All inputs are finite; a program needn't handle non-finite values.
Results may differ from the reference program's by a relative error of at most 0.006.
Values may be sent and summed in bfloat16 or wider, within the bound.
No kernel may reach another device: no remote copies, remote signals or barrier semaphores. Data moves between devices by JAX's collectives and lax.ppermute only.
A program may use at most 192 MiB of HBM per device.

```python
import jax
import jax.numpy as jnp
from jax import lax

N_EMB = 512
D = 128
RANK = 32
HID = 2048
TOKENS = 512


def draw_embeddings(key, part):
    key = jax.random.fold_in(key, 7)
    key_vals, key_emb, key_tok = jax.random.split(key, 3)
    rising = 3.0 ** (jnp.arange(N_EMB, dtype=jnp.float32) / N_EMB)
    values = jnp.clip(jax.random.normal(key_vals, (TOKENS, D, N_EMB), jnp.float32), -4.0, 4.0)
    emb_scale = rising * jnp.exp(jax.random.uniform(key_emb, (N_EMB,), jnp.float32, 0.0, jnp.log(10.0 / 3.0)))
    tok_scale = jnp.exp(jax.random.uniform(key_tok, (TOKENS,), jnp.float32, 0.0, jnp.log(3.0)))
    return (values * emb_scale[None, None, :] * tok_scale[:, None, None]).astype(jnp.bfloat16)


def steps_of(stream_key, shape, shards, smallest, top_value):
    loudness = 1.0
    for axis_at, blocks in shards:
        draws = jax.random.uniform(jax.random.fold_in(jax.random.fold_in(stream_key, 6), axis_at), (blocks,), jnp.float32, smallest / len(shards), top_value / len(shards))
        loudness = loudness * jnp.repeat(jnp.exp(draws), shape[axis_at] // blocks).reshape((-1,) + (1,) * (len(shape) - 1 - axis_at))
    return loudness


def normal_values(stream_key, extent, spread, limit, pieces=(), held_as=jnp.bfloat16):
    drawn = spread * jax.random.normal(stream_key, extent, jnp.float32)
    if pieces:
        drawn = drawn * steps_of(stream_key, extent, pieces, -0.22, 0.18)
    return jnp.clip(drawn, -limit, limit).astype(held_as)


def setup_inputs(seed: int = 0) -> dict:
    key_list = jax.random.split(jax.random.key(seed), 7)
    embeddings = draw_embeddings(jax.random.fold_in(key_list[6], 71), 0)
    projection = normal_values(key_list[1], (N_EMB, RANK), N_EMB ** -0.5, 0.25)
    w_in = normal_values(key_list[2], (N_EMB * RANK, HID), (N_EMB * RANK) ** -0.5, 0.046875, ((0, 4), (1, 2)))
    bias = normal_values(key_list[3], (HID,), 0.5, 3.0, ((0, 2),), jnp.float32)
    w_out = normal_values(key_list[4], (HID, D, N_EMB), HID ** -0.5, 0.125, ((1, 2), (2, 4)))
    cotangent = normal_values(key_list[5], (TOKENS, D, N_EMB), 0.03, 0.1796875, ((0, 4), (1, 2), (2, 4)))
    return {"embeddings": embeddings, "projection": projection, "w_in": w_in, "bias": bias, "w_out": w_out, "cotangent": cotangent}


epsilon = 1e-06

def reference(embeddings, projection, w_in, bias, w_out, cotangent):
    highest = lax.Precision.HIGHEST
    emb_float = embeddings.astype(jnp.float32)
    folded = jnp.einsum('bde,ek->bdk', emb_float, projection.astype(jnp.float32), precision=highest)
    interact = jnp.einsum('bde,bdk->bek', emb_float, folded, precision=highest)
    inv_rms = lax.rsqrt(lax.optimization_barrier(jnp.mean(interact * interact, axis=(1, 2))) + epsilon)[:, None, None]
    normed = interact * inv_rms
    activated = normed.astype(jnp.bfloat16).reshape(TOKENS, N_EMB * RANK)
    preact = jnp.dot(activated, w_in, preferred_element_type=jnp.float32) + bias
    hidden = jax.nn.silu(preact).astype(jnp.bfloat16)
    flat_out = w_out.reshape(HID, D * N_EMB)
    mixed = jnp.dot(hidden, flat_out, preferred_element_type=jnp.float32).astype(jnp.bfloat16).reshape(TOKENS, D, N_EMB)
    cot_rows = cotangent.reshape(TOKENS, D * N_EMB)
    d_hidden = lax.dot_general(cot_rows, flat_out, (((1,), (1,)), ((), ())), preferred_element_type=jnp.float32)
    sigmoid_pre = jax.nn.sigmoid(preact)
    d_preact = d_hidden * sigmoid_pre * (1.0 + preact * (1.0 - sigmoid_pre))
    d_pre_b = d_preact.astype(jnp.bfloat16)
    grad_out = lax.dot_general(hidden, cot_rows, (((0,), (0,)), ((), ())), preferred_element_type=jnp.float32).reshape(HID, D, N_EMB)
    grad_in = lax.dot_general(activated, d_pre_b, (((0,), (0,)), ((), ())), preferred_element_type=jnp.float32)
    grad_bias = lax.optimization_barrier(jnp.sum(d_preact, axis=0))
    d_act = lax.dot_general(d_pre_b, w_in, (((1,), (1,)), ((), ())), preferred_element_type=jnp.float32).reshape(TOKENS, N_EMB, RANK)
    inner_term = lax.optimization_barrier(jnp.mean(d_act * normed, axis=(1, 2)))[:, None, None]
    d_inter = (inv_rms * (d_act - normed * inner_term)).astype(jnp.bfloat16)
    back_fold = jnp.einsum('bek,bde->bdk', d_inter.astype(jnp.float32), emb_float, precision=highest)
    grad_proj = jnp.einsum('bde,bdk->ek', emb_float, back_fold, precision=highest)
    return (mixed, grad_out, grad_in, grad_bias, grad_proj)
```

```python
import jax
import jax.numpy as jnp
from jax import lax
from jax.experimental import pallas as pl
from jax.sharding import PartitionSpec as P

epsilon = 1e-06
RC = ("row", "col")
f32 = jnp.float32
bf16 = jnp.bfloat16


def dot(left, right, contract, batch=((), ())):
    return lax.dot_general(left, right, (contract, batch), preferred_element_type=f32)


def folded_ring(count):
    return list(range(0, count, 2)) + [i for i in range(count - 1, 0, -1) if i % 2]


def canonical(pieces, place):
    count = len(pieces)
    if count == 1:
        return jnp.stack(pieces)
    twice = jnp.stack(list(pieces) + list(pieces[:-1]))
    return lax.dynamic_slice_in_dim(twice, (count - place) % count, count, 0)


def grad_out_call(hidden_t, cot_blocks, embs):
    hid, _ = hidden_t.shape
    feats, toks, _ = cot_blocks[0].shape
    tile = 8

    def body(hid_ref, *refs):
        out = refs[-1].reshape(hid * tile, embs)
        for d in range(0, tile, 2):
            pair = [jnp.concatenate([b[d + i] for b in refs[:-1]], axis=0) for i in range(2)]
            res = jnp.dot(hid_ref[...], jnp.concatenate(pair, axis=1), preferred_element_type=f32)
            for i in range(2):
                out[pl.ds(d + i, hid, stride=tile), :] = res[:, i * embs : (i + 1) * embs]

    return pl.pallas_call(
        body,
        grid=(feats // tile,),
        in_specs=[pl.BlockSpec(hidden_t.shape, lambda i: (0, 0))]
        + [pl.BlockSpec((tile, toks, embs), lambda i: (i, 0, 0)) for _ in cot_blocks],
        out_specs=pl.BlockSpec((hid, tile, embs), lambda i: (0, i, 0)),
        out_shape=jax.ShapeDtypeStruct((hid, feats, embs), f32),
        cost_estimate=pl.CostEstimate(
            flops=2 * hid * hidden_t.shape[1] * feats * embs,
            transcendentals=0,
            bytes_accessed=4 * hid * feats * embs + 2 * hidden_t.shape[1] * (hid + feats * embs),
        ),
        name="grad_out",
    )(hidden_t, *cot_blocks)


def whole_step(embeddings, projection, w_in, bias, w_out, cotangent):
    toks, _, embs = embeddings.shape
    rank = projection.shape[1]
    hid = w_out.shape[0]
    rows, cols, batches = (lax.axis_size(a) for a in ("row", "col", "batch"))
    r, c, z = (lax.axis_index(a) for a in ("row", "col", "batch"))
    own = toks // (rows * cols)
    quarter = toks // rows
    hid_local = w_in.shape[1]
    flat_emb = embs * rank

    def from_rc(piece_for, jr, jc):
        piece = piece_for((r + rows - jr) % rows, (c + cols - jc) % cols, jr, jc)
        if jr == 0 and jc == 0:
            return piece
        pairs = [
            (a * cols + b, ((a - jr) % rows) * cols + (b - jc) % cols)
            for a in range(rows)
            for b in range(cols)
        ]
        return lax.ppermute(piece, RC, pairs)

    def all_from_rc(piece_for):
        if rows * cols <= 8:
            return [[from_rc(piece_for, jr, jc) for jc in range(cols)] for jr in range(rows)]
        out = [
            piece_for(a, b, (r + rows - a) % rows, (c + cols - b) % cols) for a in range(rows) for b in range(cols)
        ]
        got = lax.all_to_all(jnp.stack(out), RC, split_axis=0, concat_axis=0)
        got = got.reshape((rows, cols) + got.shape[1:])
        return [
            [
                lax.dynamic_index_in_dim(
                    lax.dynamic_index_in_dim(got, (r + jr) % rows, 0, keepdims=False), (c + jc) % cols, 0, keepdims=False
                )
                for jc in range(cols)
            ]
            for jr in range(rows)
        ]

    def from_row(piece, jr):
        if jr == 0:
            return piece
        return lax.ppermute(piece, "row", [(a, (a - jr) % rows) for a in range(rows)])

    def from_col(piece, jc):
        if jc == 0:
            return piece
        return lax.ppermute(piece, "col", [(a, (a - jc) % cols) for a in range(cols)])

    ring = folded_ring(batches)
    ring_of = jnp.asarray(ring, jnp.int32)
    place_of = jnp.asarray([ring.index(i) for i in range(batches)], jnp.int32)
    ring_place = place_of[z]

    def from_ring(piece, s):
        if s == 0:
            return piece
        return lax.ppermute(piece, "batch", [(ring[a], ring[(a + s) % batches]) for a in range(batches)])

    def ring_z(s):
        return ring_of[(ring_place + batches - s) % batches]

    cot_blocks = [jnp.transpose(cotangent, (1, 0, 2))]
    for _ in range(1, batches):
        cot_blocks.append(from_ring(cot_blocks[-1], 1))

    def emb_piece(dr, dc, jr, jc):
        return lax.dynamic_slice_in_dim(embeddings, (dr * cols + dc) * own, own, 0)

    whole = jnp.concatenate(
        [jnp.concatenate(pieces, axis=1) for pieces in all_from_rc(emb_piece)],
        axis=2,
    )
    stacked = projection.reshape(rows, embs, rank)
    turned = jnp.concatenate([stacked, stacked], axis=0)
    proj_rel = lax.dynamic_slice_in_dim(turned, r, rows, 0).reshape(rows * embs, rank)

    dh_part = jnp.transpose(dot(w_out, cotangent, ((1, 2), (1, 2))).astype(bf16))

    def dh_piece(dr, dc, jr, jc):
        return lax.dynamic_slice(dh_part, (dr * quarter, dc * hid_local), (quarter, hid_local))

    d_hidden = 0.0
    for pieces in all_from_rc(dh_piece):
        for piece in pieces:
            d_hidden = d_hidden + piece.astype(f32)

    folded = dot(whole, proj_rel, ((2,), (0,)))
    high = lax.reduce_precision(folded, 8, 7)
    both = jnp.concatenate([high.astype(bf16), (folded - high).astype(bf16)], axis=2)
    inter2 = dot(both, whole, ((1,), (1,)), ((0,), (0,)))
    interact = inter2[:, :rank] + inter2[:, rank:]
    feature_count = rank * embs * rows
    square_sum = jnp.sum(interact * interact, axis=(1, 2), keepdims=True)
    inv_rms = lax.rsqrt(square_sum / feature_count + epsilon)
    normed = interact * inv_rms
    act_own = normed.astype(bf16)

    def act_piece(dr, dc, jr, jc):
        at = ((rows - jr) % rows) * embs
        return lax.dynamic_slice_in_dim(act_own, at, embs, 2)

    act_rel = jnp.stack([canonical(pieces, c) for pieces in all_from_rc(act_piece)]).reshape(toks, rank, embs)
    act_t = jnp.transpose(act_rel, (2, 1, 0)).reshape(flat_emb, toks)

    pre_part = dot(act_t, w_in, ((0,), (0,)))
    preact = bias[None, :]
    for jr in range(rows):
        at = ((-jr) % rows) * quarter
        preact = preact + from_row(pre_part[at : at + quarter], jr)
    sig = jax.nn.sigmoid(preact)
    hidden = (preact * sig).astype(bf16)
    d_preact = d_hidden * sig * (1.0 + preact * (1.0 - sig))
    d_pre_own = d_preact.astype(bf16)
    two_own = jnp.concatenate([d_pre_own, hidden], axis=0)
    two = [from_row(two_own, jr) for jr in range(rows)]
    d_pre_rel = jnp.concatenate([t[:quarter] for t in two], axis=0)

    dact_part = dot(w_in, d_pre_rel, ((1,), (1,))).astype(bf16)
    dact_rows = jnp.transpose(dact_part.reshape(embs, rank, rows, cols, own), (2, 3, 4, 1, 0))

    def dact_piece(dr, dc, jr, jc):
        at = (rows - jr) % rows
        mine = dact_rows[at] if isinstance(jr, int) else lax.dynamic_index_in_dim(dact_rows, at, 0, keepdims=False)
        return lax.dynamic_index_in_dim(mine, dc, 0, keepdims=False)

    d_act = []
    for pieces in all_from_rc(dact_piece):
        d_act.append(sum(piece.astype(f32) for piece in pieces))
    d_act = jnp.concatenate(d_act, axis=2)
    inner = jnp.sum(d_act * normed, axis=(1, 2), keepdims=True) / feature_count
    d_inter = (inv_rms * (d_act - normed * inner)).astype(bf16)
    back = dot(d_inter, whole, ((2,), (2,)), ((0,), (0,)))
    back_high = lax.reduce_precision(back, 8, 7)
    back2 = jnp.concatenate([back_high.astype(bf16), (back - back_high).astype(bf16)], axis=1)
    proj2 = dot(back2, whole, ((0, 2), (0, 1)))
    proj_part = proj2[:rank] + proj2[rank:]
    grad_proj = 0.0
    for jr in range(rows):
        at = ((-jr) % rows) * embs
        grad_proj = grad_proj + from_row(proj_part[:, at : at + embs], jr)
    grad_proj = jnp.sum(canonical([from_col(grad_proj, jc) for jc in range(cols)], c), axis=0)
    proj_slots = jnp.zeros((batches,) + grad_proj.shape, f32)
    for s in range(batches):
        proj_slots = lax.dynamic_update_index_in_dim(proj_slots, from_ring(grad_proj, s), ring_z(s), 0)
    grad_proj = jnp.transpose(jnp.sum(proj_slots, axis=0))

    hidden_rows = canonical([t[quarter:] for t in two], r).reshape(toks, hid_local)
    hidden_all = jnp.concatenate(list(canonical([from_col(hidden_rows, jc) for jc in range(cols)], c)), axis=1)
    mixed = dot(hidden_all, w_out, ((1,), (0,))).astype(bf16)

    per_batch = hid // batches
    hidden_t = jnp.transpose(hidden_all)
    own_hidden = []
    for s in range(batches):
        dest = ring_of[(ring_place + s) % batches]
        piece = lax.dynamic_slice_in_dim(hidden_t, dest * per_batch, per_batch, 0)
        own_hidden.append(from_ring(piece, s))
    grad_out = grad_out_call(jnp.concatenate(own_hidden, axis=1), cot_blocks, embs)

    part = flat_emb // cols
    half = lax.dynamic_slice_in_dim(act_t, c * part, part, 0)
    pre_far = [d_pre_own] + [from_ring(d_pre_own, s) for s in range(1, batches)]
    pre_far, _ = lax.optimization_barrier((jnp.concatenate(pre_far, axis=0), proj_part))
    pre_rows = [from_row(pre_far, jr) for jr in range(rows)]
    act_slots = jnp.zeros((batches, flat_emb, toks), bf16)
    pre_slots = jnp.zeros((batches, toks, hid_local), bf16)
    for s in range(batches):
        if s == 0:
            act_block = act_t
        else:
            half = from_ring(half, 1)
            act_block = canonical([from_col(half, jc) for jc in range(cols)], c)
            act_block = act_block.reshape(flat_emb, toks)
        pre_block = jnp.concatenate([p[s * quarter : (s + 1) * quarter] for p in pre_rows], axis=0)
        act_slots = lax.dynamic_update_index_in_dim(act_slots, act_block, ring_z(s), 0)
        pre_slots = lax.dynamic_update_index_in_dim(pre_slots, pre_block, ring_z(s), 0)
    grad_in = dot(act_slots, pre_slots, ((0, 2), (0, 1)))
    grad_bias = jnp.sum(pre_slots.astype(f32), axis=(0, 1))
    return (mixed, grad_out, grad_in, grad_bias, grad_proj)


def solution(mesh):
    placed = (
        P("batch", "col", "row"),
        P(),
        P("row", "col"),
        P("col"),
        P(None, "col", "row"),
        P("batch", "col", "row"),
    )
    return jax.shard_map(
        whole_step,
        mesh=mesh,
        in_specs=placed,
        out_specs=(
            P("batch", "col", "row"),
            P("batch", "col", "row"),
            P("row", "col"),
            P("col"),
            P("row", None),
        ),
        check_vma=False,
    )
```
